32 devices in a mesh: rows: 8 (over z, y), cols: 4 (over x, core).
Axes of the slice: x: 2, y: 2, z: 4, core: 2. Of those that a mesh axis runs over, the one named last changes fastest.
Arguments:
- w_gate: float32 [2048, 8192], P('rows', 'cols'), may hold values from -0.1875 to 0.1875
- first_gate: float32 [2048, 8192], P('rows', 'cols'), may hold values from -6 to 6
- second_gate: float32 [2048, 8192], P('rows', 'cols'), may hold values from 0.1 to 10
- w_up: float32 [2048, 8192], P('rows', 'cols'), may hold values from -0.1875 to 0.1875
- first_up: float32 [2048, 8192], P('rows', 'cols'), may hold values from -6 to 6
- second_up: float32 [2048, 8192], P('rows', 'cols'), may hold values from 0.1 to 10
- norm_train: float32 [2048], P(('rows', 'cols')), may hold values from 0.25 to 1.75
- norm_step: float32 [2048], P(('rows', 'cols')), may hold values from -0.3 to 0.3
Outputs:
- ready_gate: bfloat16 [2048, 8192], P(None, 'cols')
- ready_up: bfloat16 [2048, 8192], P(None, 'cols')
- column_gate: float32 [8192], P('cols')
- column_up: float32 [8192], P('cols')
- serve_norm: bfloat16 [2048], replicated
- latest_gate: float32 [2048, 8192], P('rows', 'cols')
- latest_up: float32 [2048, 8192], P('rows', 'cols')
The draws below stay inside these ranges and needn't reach their ends.
All inputs are finite; a program needn't handle non-finite values. Where the reference program divides by a largest or mean magnitude, that divisor is 1e-20 or more.
Results may differ from the reference program's by a relative error of at most 0.001.
Values may be sent and summed in bfloat16 or wider, within the bound.
A program may use at most 128 MiB of HBM per device.

```python
import math
import jax
import jax.numpy as jnp
from jax import lax

D_MODEL = 2048
D_INNER = 8192


def raised(result, key, source, target, parts, factor):
    def block_of(axis_at):
        return (jnp.arange(result.shape[axis_at]) // (result.shape[axis_at] // parts)).reshape((-1,) + (1,) * (result.ndim - 1 - axis_at))

    one_side = jax.random.permutation(key, parts)[block_of(target)]
    other_side = (block_of(target) + parts // 2) % parts
    return jnp.where((block_of(source) == one_side) | (block_of(source) == other_side), factor * result, result)


def levels(key, extent, shards, low, top_value):
    factor_of, own = 1.0, jax.random.fold_in(key, 6)
    for position, shards_of in shards:
        heights = jnp.exp(jax.random.uniform(jax.random.fold_in(own, position), (shards_of,), jnp.float32, low / len(shards), top_value / len(shards)))
        factor_of = factor_of * jnp.repeat(heights, extent[position] // shards_of).reshape([-1 if axis == position else 1 for axis in range(len(extent))])
    return factor_of


def noise(stream_key, dims, scale, bound, cuts=(), held_as=jnp.bfloat16):
    entries = jax.random.normal(stream_key, dims, jnp.float32) * scale
    if len(cuts) > 0:
        entries = levels(stream_key, dims, cuts, -0.22, 0.18) * entries
    return jnp.clip(entries, min=-bound, max=bound).astype(held_as)


def gaussian_with(rng, dims, width, limit, pieces, heavy, kind=jnp.bfloat16):
    entries = width * jax.random.normal(rng, dims, jnp.float32)
    if pieces:
        entries = entries * levels(rng, dims, pieces, -0.22, 0.18)
    return jnp.clip(raised(entries, jax.random.fold_in(rng, 3), *heavy), -limit, limit).astype(kind)


def setup_inputs(seed: int = 0) -> dict:
    streams_of = jax.random.split(jax.random.key(seed), 9)
    w_gate = gaussian_with(streams_of[0], (D_MODEL, D_INNER), D_MODEL ** -0.5, 0.1875, ((0, 8), (1, 4)), (0, 1, 8, 2.0), jnp.float32)
    first_gate = noise(streams_of[1], (D_MODEL, D_INNER), 1.0, 6.0, ((0, 8), (1, 4)), jnp.float32)
    second_gate = jnp.clip(jnp.exp(math.log(10.0) - 4.6051702 * jax.random.uniform(streams_of[2], (D_MODEL, D_INNER), jnp.float32) ** levels(streams_of[2], (D_MODEL, D_INNER), ((0, 8), (1, 4)), -0.2, 0.2)), 0.1, 10.0)
    w_up = gaussian_with(streams_of[3], (D_MODEL, D_INNER), D_MODEL ** -0.5, 0.1875, ((0, 8), (1, 4)), (0, 1, 8, 2.0), jnp.float32)
    first_up = noise(streams_of[4], (D_MODEL, D_INNER), 1.0, 6.0, ((0, 8), (1, 4)), jnp.float32)
    second_up = jnp.clip(jnp.exp(math.log(10.0) - 4.6051702 * jax.random.uniform(streams_of[5], (D_MODEL, D_INNER), jnp.float32) ** levels(streams_of[5], (D_MODEL, D_INNER), ((0, 8), (1, 4)), -0.2, 0.2)), 0.1, 10.0)
    norm_train = jnp.clip(1.0 + 0.15 * jax.random.normal(streams_of[6], (D_MODEL,), jnp.float32), 0.25, 1.75)
    norm_step = jnp.clip(jax.random.uniform(streams_of[7], (D_MODEL,), jnp.float32, -0.3, 0.3) * levels(streams_of[7], (D_MODEL,), ((0, 32),), -0.4, 0.0), -0.3, 0.3)
    return dict(w_gate=w_gate, first_gate=first_gate, second_gate=second_gate, w_up=w_up, first_up=first_up, second_up=second_up, norm_train=norm_train, norm_step=norm_step)


learn_rate = 0.01
decay_rate = 0.1
tiny_value = 1e-08

def reference(w_gate, first_gate, second_gate, w_up, first_up, second_up, norm_train, norm_step):
    latest_gate = w_gate - learn_rate * (first_gate / (jnp.sqrt(second_gate) + tiny_value) + decay_rate * w_gate)
    latest_up = w_up - learn_rate * (first_up / (jnp.sqrt(second_up) + tiny_value) + decay_rate * w_up)
    column_gate = lax.optimization_barrier(jnp.sum(jnp.abs(latest_gate), axis=0)) / D_MODEL
    ready_gate = (latest_gate / column_gate).astype(jnp.bfloat16)
    column_up = lax.optimization_barrier(jnp.sum(jnp.abs(latest_up), axis=0)) / D_MODEL
    ready_up = (latest_up / column_up).astype(jnp.bfloat16)
    serve_norm = (norm_train + norm_step).astype(jnp.bfloat16)
    return (ready_gate, ready_up, column_gate, column_up, serve_norm, latest_gate, latest_up)
```

```python
import functools

import jax
import jax.numpy as jnp
from jax import lax
from jax.experimental import pallas as pl
from jax.experimental.pallas import tpu as pltpu
from jax.sharding import PartitionSpec as P

MESH = pl.DeviceIdType.MESH

learn_rate = 0.01
decay_rate = 0.1
tiny_value = 1e-08

PARTS = 4
SLAB = 32


def stepped(w, first, second):
    return w - learn_rate * (first / (jnp.sqrt(second) + tiny_value) + decay_rate * w)


def kernel(
    n_rows, n_cols, depth,
    w_g, f_g, s_g, w_u, f_u, s_u, norm_ref,
    ready, column, served, latest,
    held, sums, norms, in_sem, sum_send, sum_recv, norm_send, norm_recv, send_sem, recv_sem,
):
    row, col = lax.axis_index("rows"), lax.axis_index("cols")
    z, y = row // 2, lax.rem(row, 2)
    across = z * 2 + (1 - y)
    half = z // 2
    is_outer = lax.rem(z + half, 2) == 0
    out_z, in_z = half * 3, 1 + half
    far_in_z, far_out_z = 2 - half, 3 - half * 3
    share, width = latest.shape[1], latest.shape[2] // PARTS
    pieces = 2 * PARTS
    devices = n_rows * n_cols
    me = row * n_cols + col
    sources = ((w_g, f_g, s_g), (w_u, f_u, s_u))

    def cols_of(k):
        if isinstance(k, int):
            return pl.ds((k % PARTS) * width, width)
        return pl.ds(pl.multiple_of(lax.rem(k, PARTS) * width, width), width)

    def load(k):
        copies = [
            pltpu.make_async_copy(
                ref.at[:, cols_of(k)], held.at[i, k // PARTS, :, cols_of(k)], in_sem.at[i, k]
            )
            for i, ref in enumerate(sources[k // PARTS])
        ]
        return copies

    for k in range(2):
        for c in load(k):
            c.start()

    barrier = pltpu.get_barrier_semaphore()

    def greet(i, carry):
        other = lax.rem(me + i, devices)
        pl.semaphore_signal(
            barrier, inc=1, device_id=(other // n_cols, lax.rem(other, n_cols)), device_id_type=MESH
        )
        return carry

    lax.fori_loop(1, devices, greet, 0)

    lane = lax.broadcasted_iota(jnp.int32, norm_ref.shape, 1)
    low, high = lax.rem(me, 2) * 64, lax.rem(me, 2) * 64 + 64
    norms[me] = jnp.where((lane >= low) & (lane < high), norm_ref[...], 0.0)

    def adam(k):
        for c in load(k):
            c.wait()
        w, cs = k // PARTS, cols_of(k)

        def step(r, total):
            rs = pl.ds(pl.multiple_of(r * SLAB, SLAB), SLAB)
            new = stepped(held[0, w, rs, cs], held[1, w, rs, cs], held[2, w, rs, cs])
            latest[w, rs, cs] = new
            return total + jnp.sum(jnp.abs(new).reshape(SLAB // 8, 8, width), axis=0)

        total = lax.fori_loop(0, share // SLAB, step, jnp.zeros((8, width), jnp.float32))
        sums[k, row] = jnp.sum(total, axis=0, keepdims=True)

    def sum_copy(k, i):
        other = lax.rem(row + i, n_rows)
        return pltpu.make_async_remote_copy(
            src_ref=sums.at[k, row], dst_ref=sums.at[k, row],
            send_sem=sum_send.at[k, other], recv_sem=sum_recv.at[k, row],
            device_id=(other, col), device_id_type=MESH,
        )

    def sum_arrival(k, i):
        other = lax.rem(row + i, n_rows)
        return pltpu.make_async_remote_copy(
            src_ref=sums.at[k, other], dst_ref=sums.at[k, other],
            send_sem=sum_send.at[k, other], recv_sem=sum_recv.at[k, other],
            device_id=(other, col), device_id_type=MESH,
        )

    def scale(k):
        for i in range(1, n_rows):
            sum_arrival(k, i).wait_recv()
        w, cs = k // PARTS, cols_of(k)
        mean = jnp.sum(sums[k], axis=0) / depth
        column[w, :, cs] = mean

        def step(r, carry):
            rs = pl.ds(pl.multiple_of(r * SLAB, SLAB), SLAB)
            to = pl.ds(pl.multiple_of(row * share + r * SLAB, SLAB), SLAB)
            ready[w, to, cs] = (latest[w, rs, cs] / mean).astype(jnp.bfloat16)
            return carry

        lax.fori_loop(0, share // SLAB, step, 0)

    def block(source, k, link, slot, target):
        w = k // PARTS
        ref = ready.at[w, pl.ds(pl.multiple_of(source * share, share), share), cols_of(k)]
        return pltpu.make_async_remote_copy(
            src_ref=ref, dst_ref=ref,
            send_sem=send_sem.at[link, slot, k], recv_sem=recv_sem.at[source, k],
            device_id=(target, col), device_id_type=MESH,
        )

    def arrived(source, k):
        block(source, k, 0, 0, across).wait_recv()

    away = out_z * 2 + y
    near = in_z * 2 + y
    far_near, far_away = far_in_z * 2 + y, far_out_z * 2 + y
    near_across = in_z * 2 + (1 - y)
    away_across = out_z * 2 + (1 - y)
    far_near_across, far_away_across = far_in_z * 2 + (1 - y), far_out_z * 2 + (1 - y)

    partner = jnp.where(is_outer, near, away)

    def send_own(k):
        block(row, k, 1, 0, partner).start()
        block(row, k, 0, 0, across).start()

        @pl.when(jnp.logical_not(is_outer))
        def _():
            block(row, k, 2, 0, far_near).start()

    LAG = 2
    for k in range(pieces + LAG + 2):
        if k < pieces:
            if k + 2 < pieces:
                for c in load(k + 2):
                    c.start()
            adam(k)
        if k == 1:
            pl.semaphore_wait(barrier, devices - 1)
        if 1 <= k <= pieces:
            for i in range(1, n_rows):
                sum_copy(k - 1, i).start()
        if LAG <= k - 1 < pieces + LAG:
            scale(k - 1 - LAG)
        if 0 <= k - 2 - LAG:
            send_own(k - 2 - LAG)

    def norm_copy(i):
        other = lax.rem(me + i, devices)
        return pltpu.make_async_remote_copy(
            src_ref=norms.at[me], dst_ref=norms.at[me],
            send_sem=norm_send.at[other], recv_sem=norm_recv.at[me],
            device_id=(other // n_cols, lax.rem(other, n_cols)), device_id_type=MESH,
        )

    def norm_arrival(i):
        other = lax.rem(me + i, devices)
        return pltpu.make_async_remote_copy(
            src_ref=norms.at[other], dst_ref=norms.at[other],
            send_sem=norm_send.at[other], recv_sem=norm_recv.at[other],
            device_id=(other // n_cols, lax.rem(other, n_cols)), device_id_type=MESH,
        )

    def loop(lo, hi, f):
        def body(i, carry):
            f(i)
            return carry

        lax.fori_loop(lo, hi, body, 0)

    loop(1, devices, lambda i: norm_copy(i).start())

    @pl.when(is_outer)
    def _():
        def one(k):
            arrived(near, k)

            @pl.when(k < PARTS)
            def _():
                block(near, k, 0, 1, across).start()

            arrived(across, k)
            block(across, k, 1, 1, near).start()

        loop(0, pieces, one)

        def two(k):
            arrived(far_near, k)
            block(far_near, k, 0, 2, across).start()

        loop(0, pieces, two)

        def three(k):
            arrived(far_away, k)
            block(far_away, k, 0, 3, across).start()

        loop(0, pieces, three)

        def rest(k):
            arrived(near_across, k)
            arrived(far_near_across, k)
            arrived(far_away_across, k)
            for slot in (0, 2, 3):
                block(row, k, 0, slot, across).wait_send()
            for slot in (0, 1):
                block(row, k, 1, slot, near).wait_send()

            @pl.when(k < PARTS)
            def _():
                block(row, k, 0, 1, across).wait_send()

        loop(0, pieces, rest)

    @pl.when(jnp.logical_not(is_outer))
    def _():
        def one(k):
            arrived(away, k)
            block(away, k, 2, 1, far_near).start()
            arrived(far_near, k)
            block(far_near, k, 1, 1, away).start()
            arrived(across, k)

        loop(0, pieces, one)

        def two(k):
            block(across, k, 2, 2, far_near).start()
            arrived(far_away, k)
            block(far_away, k, 1, 2, away).start()
            block(far_away, k, 0, 1, across).start()

        loop(0, pieces, two)
        loop(PARTS, pieces, lambda k: block(across, k, 1, 3, away).start())

        def rest(k):
            arrived(away_across, k)
            arrived(far_near_across, k)
            arrived(far_away_across, k)
            for slot in (0, 1):
                block(row, k, 0, slot, across).wait_send()
            for slot in (0, 1, 2):
                block(row, k, 1, slot, away).wait_send()
                block(row, k, 2, slot, far_near).wait_send()

            @pl.when(k >= PARTS)
            def _():
                block(row, k, 1, 3, away).wait_send()

        loop(0, pieces, rest)

    for k in range(pieces):
        loop(1, n_rows, lambda i: sum_copy(k, i).wait_send())
    loop(1, devices, lambda i: (norm_copy(i).wait_send(), norm_arrival(i).wait_recv()))
    for i in range(devices // 2):
        served[pl.ds(i, 1), :] = norms[2 * i][0:1] + norms[2 * i + 1][0:1]


def fused(n_rows, n_cols, w_gate, first_gate, second_gate, w_up, first_up, second_up, norm_train, norm_step):
    share, width = w_gate.shape
    depth = share * n_rows
    pieces = 2 * PARTS
    devices = n_rows * n_cols
    norm = norm_train + norm_step
    norm = jnp.broadcast_to(jnp.concatenate([norm, norm])[None, :], (8, 128))
    vmem = pl.BlockSpec(memory_space=pltpu.VMEM)
    dma = pltpu.SemaphoreType.DMA
    ready, column, served, latest = pl.pallas_call(
        functools.partial(kernel, n_rows, n_cols, depth),
        out_shape=[
            pltpu.VMEM((2, depth, width), jnp.bfloat16),
            pltpu.VMEM((2, 1, width), jnp.float32),
            pltpu.VMEM((devices // 2, 128), jnp.float32),
            pltpu.VMEM((2, share, width), jnp.float32),
        ],
        in_specs=[pl.BlockSpec(memory_space=pltpu.HBM)] * 6 + [vmem],
        out_specs=[vmem] * 4,
        scratch_shapes=[
            pltpu.VMEM((3, 2, share, width), jnp.float32),
            pltpu.VMEM((pieces, n_rows, 1, width // PARTS), jnp.float32),
            pltpu.VMEM((devices, 8, 128), jnp.float32),
            dma((3, pieces)),
            dma((pieces, n_rows)),
            dma((pieces, n_rows)),
            dma((devices,)),
            dma((devices,)),
            dma((3, 4, pieces)),
            dma((n_rows, pieces)),
        ],
        compiler_params=pltpu.CompilerParams(
            collective_id=0, has_side_effects=True, vmem_limit_bytes=40 * 2**20
        ),
        name="fused",
    )(w_gate, first_gate, second_gate, w_up, first_up, second_up, norm)
    return (
        ready[0], ready[1], column[0, 0], column[1, 0],
        served.reshape(-1).astype(jnp.bfloat16), latest[0], latest[1],
    )


def plain(n_rows, n_cols, w_gate, first_gate, second_gate, w_up, first_up, second_up, norm_train, norm_step):
    latest = [stepped(w_gate, first_gate, second_gate), stepped(w_up, first_up, second_up)]
    totals = lax.psum(tuple(jnp.sum(jnp.abs(a), axis=0) for a in latest), "rows")
    columns = [t / (w_gate.shape[0] * n_rows) for t in totals]
    ready = [
        lax.all_gather((a / c).astype(jnp.bfloat16), "rows", axis=0, tiled=True)
        for a, c in zip(latest, columns)
    ]
    served = lax.all_gather(
        (norm_train + norm_step).astype(jnp.bfloat16), ("rows", "cols"), axis=0, tiled=True
    )
    return (*ready, *columns, served, *latest)


def solution(mesh):
    n_rows, n_cols = mesh.shape["rows"], mesh.shape["cols"]
    body = fused if (n_rows, n_cols) == (8, 4) else plain
    placed = (P("rows", "cols"),) * 6 + (P(("rows", "cols")),) * 2
    return jax.shard_map(
        functools.partial(body, n_rows, n_cols),
        mesh=mesh,
        in_specs=placed,
        out_specs=(
            P(None, "cols"), P(None, "cols"), P("cols"), P("cols"), P(),
            P("rows", "cols"), P("rows", "cols"),
        ),
        check_vma=False,
    )
```

```python
import functools

import jax
import jax.numpy as jnp
from jax import lax
from jax.experimental import pallas as pl
from jax.experimental.pallas import tpu as pltpu
from jax.sharding import PartitionSpec as P

MESH = pl.DeviceIdType.MESH

learn_rate = 0.01
decay_rate = 0.1
tiny_value = 1e-08

PARTS = 8
SLAB = 64


def stepped(w, first, second):
    return w - learn_rate * (first / (jnp.sqrt(second) + tiny_value) + decay_rate * w)


def kernel(
    n_rows, n_cols, depth,
    w_g, f_g, s_g, w_u, f_u, s_u, norm_a, norm_b,
    ready, column, served, latest,
    held, sums, norms, in_sem, sum_send, sum_recv, norm_send, norm_recv, group_send, group_recv,
    send_sem, recv_sem,
):
    row, col = lax.axis_index("rows"), lax.axis_index("cols")
    z, y = row // 2, lax.rem(row, 2)
    across = z * 2 + (1 - y)
    half = z // 2
    is_outer = lax.rem(z + half, 2) == 0
    out_z, in_z = half * 3, 1 + half
    far_in_z, far_out_z = 2 - half, 3 - half * 3
    share, width = latest.shape[1], latest.shape[2] // PARTS
    pieces = 2 * PARTS
    me = row * n_cols + col
    sources = ((w_g, f_g, s_g), (w_u, f_u, s_u))

    def cols_of(k):
        if isinstance(k, int):
            return pl.ds((k % PARTS) * width, width)
        return pl.ds(pl.multiple_of(lax.rem(k, PARTS) * width, width), width)

    def load(k):
        copies = [
            pltpu.make_async_copy(
                ref.at[:, cols_of(k)], held.at[i, k // PARTS, :, cols_of(k)], in_sem.at[i, k]
            )
            for i, ref in enumerate(sources[k // PARTS])
        ]
        return copies

    for k in range(2):
        for c in load(k):
            c.start()

    barrier = pltpu.get_barrier_semaphore()

    def loop(lo, hi, f):
        def body(i, carry):
            f(i)
            return carry

        lax.fori_loop(lo, hi, body, 0)

    def row_peer(i):
        return lax.rem(row + i, n_rows)

    def col_peer(i):
        return lax.rem(col + i, n_cols)

    for i in range(1, n_rows):
        pl.semaphore_signal(barrier, inc=1, device_id=(row_peer(i), col), device_id_type=MESH)
    for i in range(1, n_cols):
        pl.semaphore_signal(barrier, inc=1, device_id=(row, col_peer(i)), device_id_type=MESH)

    lanes = norm_a.shape[1]
    norms[row, col] = jnp.zeros((1, 2 * lanes), jnp.float32)
    for side in range(2):

        @pl.when(lax.rem(me, 2) == side)
        def _():
            norms[row, col, :, side * lanes : (side + 1) * lanes] = norm_a[...] + norm_b[...]

    def adam(k):
        for c in load(k):
            c.wait()
        w, cs = k // PARTS, cols_of(k)

        def step(r, total):
            rs = pl.ds(pl.multiple_of(r * SLAB, SLAB), SLAB)
            new = stepped(held[0, w, rs, cs], held[1, w, rs, cs], held[2, w, rs, cs])
            latest[w, rs, cs] = new
            return total + jnp.sum(jnp.abs(new).reshape(SLAB // 8, 8, width), axis=0)

        total = lax.fori_loop(0, share // SLAB, step, jnp.zeros((8, width), jnp.float32))
        sums[k, row] = jnp.sum(total, axis=0, keepdims=True)

    def sum_copy(k, i):
        other = lax.rem(row + i, n_rows)
        return pltpu.make_async_remote_copy(
            src_ref=sums.at[k, row], dst_ref=sums.at[k, row],
            send_sem=sum_send.at[k, other], recv_sem=sum_recv.at[k, row],
            device_id=(other, col), device_id_type=MESH,
        )

    def sum_arrival(k, i):
        other = lax.rem(row + i, n_rows)
        return pltpu.make_async_remote_copy(
            src_ref=sums.at[k, other], dst_ref=sums.at[k, other],
            send_sem=sum_send.at[k, other], recv_sem=sum_recv.at[k, other],
            device_id=(other, col), device_id_type=MESH,
        )

    def scale(k):
        for i in range(1, n_rows):
            sum_arrival(k, i).wait_recv()
        w, cs = k // PARTS, cols_of(k)
        mean = jnp.sum(sums[k], axis=0) / depth
        column[w, :, cs] = mean

        def step(r, carry):
            rs = pl.ds(pl.multiple_of(r * SLAB, SLAB), SLAB)
            to = pl.ds(pl.multiple_of(row * share + r * SLAB, SLAB), SLAB)
            ready[w, to, cs] = (latest[w, rs, cs] / mean).astype(jnp.bfloat16)
            return carry

        lax.fori_loop(0, share // SLAB, step, 0)

    def block(source, k, link, slot, target):
        w = k // PARTS
        ref = ready.at[w, pl.ds(pl.multiple_of(source * share, share), share), cols_of(k)]
        return pltpu.make_async_remote_copy(
            src_ref=ref, dst_ref=ref,
            send_sem=send_sem.at[link, slot, k], recv_sem=recv_sem.at[source, k],
            device_id=(target, col), device_id_type=MESH,
        )

    def arrived(source, k):
        block(source, k, 0, 0, across).wait_recv()

    away = out_z * 2 + y
    near = in_z * 2 + y
    far_near, far_away = far_in_z * 2 + y, far_out_z * 2 + y
    near_across = in_z * 2 + (1 - y)
    away_across = out_z * 2 + (1 - y)
    far_near_across, far_away_across = far_in_z * 2 + (1 - y), far_out_z * 2 + (1 - y)

    partner = jnp.where(is_outer, near, away)

    def send_own(k):
        block(row, k, 1, 0, partner).start()
        block(row, k, 0, 0, across).start()

        @pl.when(jnp.logical_not(is_outer))
        def _():
            block(row, k, 2, 0, far_near).start()

    LAG = 4
    for k in range(pieces + LAG + 2):
        if k < pieces:
            if k + 2 < pieces:
                for c in load(k + 2):
                    c.start()
            adam(k)
        if k == 1:
            pl.semaphore_wait(barrier, n_rows + n_cols - 2)
        if 1 <= k <= pieces:
            for i in range(1, n_rows):
                sum_copy(k - 1, i).start()
        if LAG <= k - 1 < pieces + LAG:
            scale(k - 1 - LAG)
        if 0 <= k - 2 - LAG:
            send_own(k - 2 - LAG)

    def norm_copy(i, mine):
        at = col if mine else col_peer(i)
        return pltpu.make_async_remote_copy(
            src_ref=norms.at[row, at], dst_ref=norms.at[row, at],
            send_sem=norm_send.at[i], recv_sem=norm_recv.at[at],
            device_id=(row, col_peer(i)), device_id_type=MESH,
        )

    def group_copy(i, mine):
        at = row if mine else row_peer(i)
        return pltpu.make_async_remote_copy(
            src_ref=norms.at[at], dst_ref=norms.at[at],
            send_sem=group_send.at[i], recv_sem=group_recv.at[at],
            device_id=(row_peer(i), col), device_id_type=MESH,
        )

    for i in range(1, n_cols):
        norm_copy(i, True).start()
    for i in range(1, n_cols):
        norm_copy(i, False).wait_recv()
    for i in range(1, n_rows):
        group_copy(i, True).start()

    @pl.when(is_outer)
    def _():
        def one(k):
            arrived(near, k)

            @pl.when(k < PARTS)
            def _():
                block(near, k, 0, 1, across).start()

            arrived(across, k)
            block(across, k, 1, 1, near).start()

        loop(0, pieces, one)

        def two(k):
            arrived(far_near, k)
            block(far_near, k, 0, 2, across).start()

        loop(0, pieces, two)

        def three(k):
            arrived(far_away, k)
            block(far_away, k, 0, 3, across).start()

        loop(0, pieces, three)

        def rest(k):
            arrived(near_across, k)
            arrived(far_near_across, k)
            arrived(far_away_across, k)
            for slot in (0, 2, 3):
                block(row, k, 0, slot, across).wait_send()
            for slot in (0, 1):
                block(row, k, 1, slot, near).wait_send()

            @pl.when(k < PARTS)
            def _():
                block(row, k, 0, 1, across).wait_send()

        loop(0, pieces, rest)

    @pl.when(jnp.logical_not(is_outer))
    def _():
        def one(k):
            arrived(away, k)
            block(away, k, 2, 1, far_near).start()
            arrived(far_near, k)
            block(far_near, k, 1, 1, away).start()
            arrived(across, k)

        loop(0, pieces, one)

        def two(k):
            block(across, k, 2, 2, far_near).start()
            arrived(far_away, k)
            block(far_away, k, 1, 2, away).start()
            block(far_away, k, 0, 1, across).start()

        loop(0, pieces, two)
        loop(PARTS, pieces, lambda k: block(across, k, 1, 3, away).start())

        def rest(k):
            arrived(away_across, k)
            arrived(far_near_across, k)
            arrived(far_away_across, k)
            for slot in (0, 1):
                block(row, k, 0, slot, across).wait_send()
            for slot in (0, 1, 2):
                block(row, k, 1, slot, away).wait_send()
                block(row, k, 2, slot, far_near).wait_send()

            @pl.when(k >= PARTS)
            def _():
                block(row, k, 1, 3, away).wait_send()

        loop(0, pieces, rest)

    for k in range(pieces):
        loop(1, n_rows, lambda i: sum_copy(k, i).wait_send())
    for i in range(1, n_cols):
        norm_copy(i, True).wait_send()
    for i in range(1, n_rows):
        group_copy(i, True).wait_send()
        group_copy(i, False).wait_recv()
    pairs = n_cols // 2
    for i in range(n_rows * pairs):
        r, c = i // pairs, 2 * (i % pairs)
        served[pl.ds(i, 1), :] = norms[r, c] + norms[r, c + 1]


def finish(ready, column, served, latest, *rest):
    outs, narrow, sem = rest[:7], rest[7], rest[8]
    narrow[...] = served[...].astype(jnp.bfloat16)
    copies = []
    cuts = 4
    rows = ready.shape[1] // cuts
    for w in range(2):
        for i in range(cuts):
            at = pl.ds(i * rows, rows)
            copies.append((ready.at[w, at], outs[w].at[at]))
        copies.append((latest.at[w], outs[5 + w]))
        copies.append((column.at[w], outs[2 + w]))
    copies.append((narrow, outs[4]))
    started = [pltpu.make_async_copy(a, b, sem.at[i]) for i, (a, b) in enumerate(copies)]
    for c in started:
        c.start()
    for c in started:
        c.wait()


def fused(n_rows, n_cols, w_gate, first_gate, second_gate, w_up, first_up, second_up, norm_train, norm_step):
    share, width = w_gate.shape
    depth = share * n_rows
    pieces = 2 * PARTS
    lines = n_rows * n_cols // 2
    lanes = norm_train.shape[0]
    vmem = pl.BlockSpec(memory_space=pltpu.VMEM)
    hbm = pl.BlockSpec(memory_space=pltpu.HBM)
    dma = pltpu.SemaphoreType.DMA
    found = pl.pallas_call(
        functools.partial(kernel, n_rows, n_cols, depth),
        out_shape=[
            pltpu.VMEM((2, depth, width), jnp.bfloat16),
            pltpu.VMEM((2, 1, width), jnp.float32),
            pltpu.VMEM((lines, 2 * lanes), jnp.float32),
            pltpu.VMEM((2, share, width), jnp.float32),
        ],
        in_specs=[hbm] * 6 + [vmem] * 2,
        out_specs=[vmem] * 4,
        scratch_shapes=[
            pltpu.VMEM((3, 2, share, width), jnp.float32),
            pltpu.VMEM((pieces, n_rows, 1, width // PARTS), jnp.float32),
            pltpu.VMEM((n_rows, n_cols, 1, 2 * lanes), jnp.float32),
            dma((3, pieces)),
            dma((pieces, n_rows)),
            dma((pieces, n_rows)),
            dma((n_cols,)),
            dma((n_cols,)),
            dma((n_rows,)),
            dma((n_rows,)),
            dma((3, 4, pieces)),
            dma((n_rows, pieces)),
        ],
        compiler_params=pltpu.CompilerParams(
            collective_id=0, has_side_effects=True, vmem_limit_bytes=36 * 2**20
        ),
        name="fused",
    )(
        w_gate, first_gate, second_gate, w_up, first_up, second_up,
        norm_train.reshape(1, -1), norm_step.reshape(1, -1),
    )
    ready_gate, ready_up, column_gate, column_up, served, latest_gate, latest_up = pl.pallas_call(
        finish,
        out_shape=[jax.ShapeDtypeStruct((depth, width), jnp.bfloat16)] * 2
        + [jax.ShapeDtypeStruct((1, width), jnp.float32)] * 2
        + [jax.ShapeDtypeStruct((lines, 2 * lanes), jnp.bfloat16)]
        + [jax.ShapeDtypeStruct((share, width), jnp.float32)] * 2,
        in_specs=[vmem] * 4,
        out_specs=[hbm] * 7,
        scratch_shapes=[pltpu.VMEM((lines, 2 * lanes), jnp.bfloat16), dma((13,))],
        compiler_params=pltpu.CompilerParams(vmem_limit_bytes=2**20),
        name="finish",
    )(*found)
    return (
        ready_gate, ready_up, column_gate.reshape(-1), column_up.reshape(-1), served.reshape(-1),
        latest_gate, latest_up,
    )


def plain(n_rows, n_cols, w_gate, first_gate, second_gate, w_up, first_up, second_up, norm_train, norm_step):
    latest = [stepped(w_gate, first_gate, second_gate), stepped(w_up, first_up, second_up)]
    totals = lax.psum(tuple(jnp.sum(jnp.abs(a), axis=0) for a in latest), "rows")
    columns = [t / (w_gate.shape[0] * n_rows) for t in totals]
    ready = [
        lax.all_gather((a / c).astype(jnp.bfloat16), "rows", axis=0, tiled=True)
        for a, c in zip(latest, columns)
    ]
    served = lax.all_gather(
        (norm_train + norm_step).astype(jnp.bfloat16), ("rows", "cols"), axis=0, tiled=True
    )
    return (*ready, *columns, served, *latest)


def solution(mesh):
    n_rows, n_cols = mesh.shape["rows"], mesh.shape["cols"]
    body = fused if (n_rows, n_cols) == (8, 4) else plain
    placed = (P("rows", "cols"),) * 6 + (P(("rows", "cols")),) * 2
    return jax.shard_map(
        functools.partial(body, n_rows, n_cols),
        mesh=mesh,
        in_specs=placed,
        out_specs=(
            P(None, "cols"), P(None, "cols"), P("cols"), P("cols"), P(),
            P("rows", "cols"), P("rows", "cols"),
        ),
        check_vma=False,
    )
```

```python
import functools

import jax
import jax.numpy as jnp
from jax import lax
from jax.experimental import pallas as pl
from jax.experimental.pallas import tpu as pltpu
from jax.sharding import PartitionSpec as P

MESH = pl.DeviceIdType.MESH

learn_rate = 0.01
decay_rate = 0.1
tiny_value = 1e-08

PARTS = 8
LATE = 2
SLAB = 64


def stepped(w, first, second):
    return w - learn_rate * (first / (jnp.sqrt(second) + tiny_value) + decay_rate * w)


def kernel(
    n_rows, n_cols, depth,
    w_g, f_g, s_g, w_u, f_u, s_u, norm_a, norm_b,
    ready, column, served, latest, late,
    held, sums, norms, in_sem, sum_send, sum_recv, norm_send, norm_recv, group_send, group_recv,
    send_sem, recv_sem,
):
    row, col = lax.axis_index("rows"), lax.axis_index("cols")
    z, y = row // 2, lax.rem(row, 2)
    across = z * 2 + (1 - y)
    half = z // 2
    is_outer = lax.rem(z + half, 2) == 0
    out_z, in_z = half * 3, 1 + half
    far_in_z, far_out_z = 2 - half, 3 - half * 3
    share, width = latest.shape[1], latest.shape[2] // PARTS
    pieces = 2 * PARTS
    me = row * n_cols + col
    sources = ((w_g, f_g, s_g), (w_u, f_u, s_u))

    def cols_of(k):
        if isinstance(k, int):
            return pl.ds((k % PARTS) * width, width)
        return pl.ds(pl.multiple_of(lax.rem(k, PARTS) * width, width), width)

    def load(k):
        copies = [
            pltpu.make_async_copy(
                ref.at[:, cols_of(k)], held.at[i, k // PARTS, :, cols_of(k)], in_sem.at[i, k]
            )
            for i, ref in enumerate(sources[k // PARTS])
        ]
        return copies

    for k in range(2):
        for c in load(k):
            c.start()

    barrier = pltpu.get_barrier_semaphore()

    def loop(lo, hi, f):
        def body(i, carry):
            f(i)
            return carry

        lax.fori_loop(lo, hi, body, 0)

    def row_peer(i):
        return lax.rem(row + i, n_rows)

    def col_peer(i):
        return lax.rem(col + i, n_cols)

    for i in range(1, n_rows):
        pl.semaphore_signal(barrier, inc=1, device_id=(row_peer(i), col), device_id_type=MESH)
    for i in range(1, n_cols):
        pl.semaphore_signal(barrier, inc=1, device_id=(row, col_peer(i)), device_id_type=MESH)

    lanes = norm_a.shape[1]
    norms[row, col] = jnp.zeros((1, 2 * lanes), jnp.float32)
    for side in range(2):

        @pl.when(lax.rem(me, 2) == side)
        def _():
            norms[row, col, :, side * lanes : (side + 1) * lanes] = norm_a[...] + norm_b[...]

    def adam(k):
        for c in load(k):
            c.wait()
        w, cs = k // PARTS, cols_of(k)

        def step(r, total):
            rs = pl.ds(pl.multiple_of(r * SLAB, SLAB), SLAB)
            new = stepped(held[0, w, rs, cs], held[1, w, rs, cs], held[2, w, rs, cs])
            latest[w, rs, cs] = new
            return total + jnp.sum(jnp.abs(new).reshape(SLAB // 8, 8, width), axis=0)

        total = lax.fori_loop(0, share // SLAB, step, jnp.zeros((8, width), jnp.float32))
        sums[k, row] = jnp.sum(total, axis=0, keepdims=True)

    def sum_copy(k, i):
        other = lax.rem(row + i, n_rows)
        return pltpu.make_async_remote_copy(
            src_ref=sums.at[k, row], dst_ref=sums.at[k, row],
            send_sem=sum_send.at[k, other], recv_sem=sum_recv.at[k, row],
            device_id=(other, col), device_id_type=MESH,
        )

    def sum_arrival(k, i):
        other = lax.rem(row + i, n_rows)
        return pltpu.make_async_remote_copy(
            src_ref=sums.at[k, other], dst_ref=sums.at[k, other],
            send_sem=sum_send.at[k, other], recv_sem=sum_recv.at[k, other],
            device_id=(other, col), device_id_type=MESH,
        )

    def scale(k):
        for i in range(1, n_rows):
            sum_arrival(k, i).wait_recv()
        w, cs = k // PARTS, cols_of(k)
        mean = jnp.sum(sums[k], axis=0) / depth
        column[w, :, cs] = mean

        def step(r, carry):
            rs = pl.ds(pl.multiple_of(r * SLAB, SLAB), SLAB)
            to = pl.ds(pl.multiple_of(row * share + r * SLAB, SLAB), SLAB)
            ready[w, to, cs] = (latest[w, rs, cs] / mean).astype(jnp.bfloat16)
            return carry

        lax.fori_loop(0, share // SLAB, step, 0)

    def block(source, k, link, slot, target):
        w = k // PARTS
        ref = ready.at[w, pl.ds(pl.multiple_of(source * share, share), share), cols_of(k)]
        return pltpu.make_async_remote_copy(
            src_ref=ref, dst_ref=ref,
            send_sem=send_sem.at[link, slot, k], recv_sem=recv_sem.at[source, k],
            device_id=(target, col), device_id_type=MESH,
        )

    def arrived(source, k):
        block(source, k, 0, 0, across).wait_recv()

    away = out_z * 2 + y
    near = in_z * 2 + y
    far_near, far_away = far_in_z * 2 + y, far_out_z * 2 + y
    near_across = in_z * 2 + (1 - y)
    away_across = out_z * 2 + (1 - y)
    far_near_across, far_away_across = far_in_z * 2 + (1 - y), far_out_z * 2 + (1 - y)

    partner = jnp.where(is_outer, near, away)

    def send_own(k):
        block(row, k, 1, 0, partner).start()
        block(row, k, 0, 0, across).start()

        @pl.when(jnp.logical_not(is_outer))
        def _():
            block(row, k, 2, 0, far_near).start()

    LAG = 4
    for k in range(pieces + LAG + 1):
        if k < pieces:
            if k + 2 < pieces:
                for c in load(k + 2):
                    c.start()
            adam(k)
        if k == 1:
            pl.semaphore_wait(barrier, n_rows + n_cols - 2)
        if 0 <= k - 1 - LAG:
            scale(k - 1 - LAG)
        if 1 <= k <= pieces:
            for i in range(1, n_rows):
                sum_copy(k - 1, i).start()
        if 0 <= k - 1 - LAG:
            send_own(k - 1 - LAG)

    def norm_copy(i, mine):
        at = col if mine else col_peer(i)
        return pltpu.make_async_remote_copy(
            src_ref=norms.at[row, at], dst_ref=norms.at[row, at],
            send_sem=norm_send.at[i], recv_sem=norm_recv.at[at],
            device_id=(row, col_peer(i)), device_id_type=MESH,
        )

    def group_copy(i, mine):
        at = row if mine else row_peer(i)
        return pltpu.make_async_remote_copy(
            src_ref=norms.at[at], dst_ref=norms.at[at],
            send_sem=group_send.at[i], recv_sem=group_recv.at[at],
            device_id=(row_peer(i), col), device_id_type=MESH,
        )

    for i in range(1, n_cols):
        norm_copy(i, True).start()
    for i in range(1, n_cols):
        norm_copy(i, False).wait_recv()
    for i in range(1, n_rows):
        group_copy(i, True).start()

    def keep(source):
        at = pl.ds(pl.multiple_of(source * share, share), share)
        late[...] = ready[1, at, (PARTS - LATE) * width : PARTS * width]

    @pl.when(is_outer)
    def _():
        def one(k):
            arrived(near, k)

            @pl.when(k < PARTS)
            def _():
                block(near, k, 0, 1, across).start()

            arrived(across, k)
            block(across, k, 1, 1, near).start()

        loop(0, pieces, one)

        def two(k):
            arrived(far_near, k)
            block(far_near, k, 0, 2, across).start()

        loop(0, pieces, two)

        def three(k):
            arrived(far_away, k)

            @pl.when(k < pieces - LATE)
            def _():
                block(far_away, k, 0, 3, across).start()

        loop(0, pieces, three)
        keep(far_away)

        def rest(k):
            arrived(far_near_across, k)

            @pl.when(k < pieces - LATE)
            def _():
                arrived(near_across, k)
                arrived(far_away_across, k)
                block(row, k, 0, 3, across).wait_send()

            for slot in (0, 2):
                block(row, k, 0, slot, across).wait_send()
            for slot in (0, 1):
                block(row, k, 1, slot, near).wait_send()

            @pl.when(k < PARTS)
            def _():
                block(row, k, 0, 1, across).wait_send()

        loop(0, pieces, rest)

    @pl.when(jnp.logical_not(is_outer))
    def _():
        def one(k):
            arrived(away, k)
            block(away, k, 2, 1, far_near).start()
            arrived(far_near, k)
            block(far_near, k, 1, 1, away).start()
            arrived(across, k)

        loop(0, pieces, one)

        def two(k):
            block(across, k, 2, 2, far_near).start()
            arrived(far_away, k)
            block(far_away, k, 1, 2, away).start()
            block(far_away, k, 0, 1, across).start()

        loop(0, pieces, two)
        loop(PARTS, pieces - LATE, lambda k: block(across, k, 1, 3, away).start())
        keep(across)

        def rest(k):
            arrived(away_across, k)
            arrived(far_near_across, k)
            arrived(far_away_across, k)
            for slot in (0, 1):
                block(row, k, 0, slot, across).wait_send()
            for slot in (0, 1, 2):
                block(row, k, 1, slot, away).wait_send()
                block(row, k, 2, slot, far_near).wait_send()

            @pl.when((k >= PARTS) & (k < pieces - LATE))
            def _():
                block(row, k, 1, 3, away).wait_send()

        loop(0, pieces, rest)

    for k in range(pieces):
        loop(1, n_rows, lambda i: sum_copy(k, i).wait_send())
    for i in range(1, n_cols):
        norm_copy(i, True).wait_send()
    for i in range(1, n_rows):
        group_copy(i, True).wait_send()
        group_copy(i, False).wait_recv()
    pairs = n_cols // 2
    for i in range(n_rows * pairs):
        r, c = i // pairs, 2 * (i % pairs)
        served[pl.ds(i, 1), :] = norms[r, c] + norms[r, c + 1]


def finish(ready, column, served, latest, *rest):
    outs, narrow, sem = rest[:7], rest[7], rest[8]
    narrow[...] = served[...].astype(jnp.bfloat16)
    copies = []
    cuts = 4
    rows = ready.shape[1] // cuts
    for w in range(2):
        for i in range(cuts):
            at = pl.ds(i * rows, rows)
            copies.append((ready.at[w, at], outs[w].at[at]))
        copies.append((latest.at[w], outs[5 + w]))
        copies.append((column.at[w], outs[2 + w]))
    copies.append((narrow, outs[4]))
    started = [pltpu.make_async_copy(a, b, sem.at[i]) for i, (a, b) in enumerate(copies)]
    for c in started:
        c.start()
    for c in started:
        c.wait()


def place(from_z, from_y, old, new, sem):
    row = lax.axis_index("rows")
    z, y = row // 2, lax.rem(row, 2)
    half = z // 2
    share, width = from_z.shape

    @pl.when(lax.rem(z + half, 2) == 0)
    def _():
        copies = []
        for i, (ref, at_z) in enumerate(((from_z, 1 + half), (from_y, 3 - half * 3))):
            start = pl.multiple_of((at_z * 2 + 1 - y) * share, share)
            to = new.at[pl.ds(start, share), pl.ds(new.shape[1] - width, width)]
            copies.append(pltpu.make_async_copy(ref, to, sem.at[i]))
        for c in copies:
            c.start()
        for c in copies:
            c.wait()


def fused(n_rows, n_cols, w_gate, first_gate, second_gate, w_up, first_up, second_up, norm_train, norm_step):
    share, width = w_gate.shape
    depth = share * n_rows
    pieces = 2 * PARTS
    lines = n_rows * n_cols // 2
    lanes = norm_train.shape[0]
    vmem = pl.BlockSpec(memory_space=pltpu.VMEM)
    hbm = pl.BlockSpec(memory_space=pltpu.HBM)
    dma = pltpu.SemaphoreType.DMA
    *found, late = pl.pallas_call(
        functools.partial(kernel, n_rows, n_cols, depth),
        out_shape=[
            pltpu.VMEM((2, depth, width), jnp.bfloat16),
            pltpu.VMEM((2, 1, width), jnp.float32),
            pltpu.VMEM((lines, 2 * lanes), jnp.float32),
            pltpu.VMEM((2, share, width), jnp.float32),
            pltpu.VMEM((share, LATE * (width // PARTS)), jnp.bfloat16),
        ],
        in_specs=[hbm] * 6 + [vmem] * 2,
        out_specs=[vmem] * 5,
        scratch_shapes=[
            pltpu.VMEM((3, 2, share, width), jnp.float32),
            pltpu.VMEM((pieces, n_rows, 1, width // PARTS), jnp.float32),
            pltpu.VMEM((n_rows, n_cols, 1, 2 * lanes), jnp.float32),
            dma((3, pieces)),
            dma((pieces, n_rows)),
            dma((pieces, n_rows)),
            dma((n_cols,)),
            dma((n_cols,)),
            dma((n_rows,)),
            dma((n_rows,)),
            dma((3, 4, pieces)),
            dma((n_rows, pieces)),
        ],
        compiler_params=pltpu.CompilerParams(
            collective_id=0, has_side_effects=True, vmem_limit_bytes=36 * 2**20
        ),
        name="fused",
    )(
        w_gate, first_gate, second_gate, w_up, first_up, second_up,
        norm_train.reshape(1, -1), norm_step.reshape(1, -1),
    )
    last = n_rows - 1
    from_z = lax.ppermute(late, "rows", [(2, 0), (3, 1), (last - 3, last - 1), (last - 2, last)])
    from_y = lax.ppermute(late, "rows", [(0, 1), (1, 0), (last - 1, last), (last, last - 1)])
    ready_gate, ready_up, column_gate, column_up, served, latest_gate, latest_up = pl.pallas_call(
        finish,
        out_shape=[jax.ShapeDtypeStruct((depth, width), jnp.bfloat16)] * 2
        + [jax.ShapeDtypeStruct((1, width), jnp.float32)] * 2
        + [jax.ShapeDtypeStruct((lines, 2 * lanes), jnp.bfloat16)]
        + [jax.ShapeDtypeStruct((share, width), jnp.float32)] * 2,
        in_specs=[vmem] * 4,
        out_specs=[hbm] * 7,
        scratch_shapes=[pltpu.VMEM((lines, 2 * lanes), jnp.bfloat16), dma((13,))],
        compiler_params=pltpu.CompilerParams(vmem_limit_bytes=2**20),
        cost_estimate=pl.CostEstimate(flops=0, bytes_accessed=40 * 2**20, transcendentals=0),
        name="finish",
    )(*found)
    ready_up = pl.pallas_call(
        place,
        out_shape=jax.ShapeDtypeStruct((depth, width), jnp.bfloat16),
        in_specs=[vmem] * 2 + [hbm],
        out_specs=hbm,
        input_output_aliases={2: 0},
        scratch_shapes=[dma((2,))],
        compiler_params=pltpu.CompilerParams(vmem_limit_bytes=2**20),
        name="place",
    )(from_z, from_y, ready_up)
    return (
        ready_gate, ready_up, column_gate.reshape(-1), column_up.reshape(-1), served.reshape(-1),
        latest_gate, latest_up,
    )


def plain(n_rows, n_cols, w_gate, first_gate, second_gate, w_up, first_up, second_up, norm_train, norm_step):
    latest = [stepped(w_gate, first_gate, second_gate), stepped(w_up, first_up, second_up)]
    totals = lax.psum(tuple(jnp.sum(jnp.abs(a), axis=0) for a in latest), "rows")
    columns = [t / (w_gate.shape[0] * n_rows) for t in totals]
    ready = [
        lax.all_gather((a / c).astype(jnp.bfloat16), "rows", axis=0, tiled=True)
        for a, c in zip(latest, columns)
    ]
    served = lax.all_gather(
        (norm_train + norm_step).astype(jnp.bfloat16), ("rows", "cols"), axis=0, tiled=True
    )
    return (*ready, *columns, served, *latest)


def solution(mesh):
    n_rows, n_cols = mesh.shape["rows"], mesh.shape["cols"]
    body = fused if (n_rows, n_cols) == (8, 4) else plain
    placed = (P("rows", "cols"),) * 6 + (P(("rows", "cols")),) * 2
    return jax.shard_map(
        functools.partial(body, n_rows, n_cols),
        mesh=mesh,
        in_specs=placed,
        out_specs=(
            P(None, "cols"), P(None, "cols"), P("cols"), P("cols"), P(),
            P("rows", "cols"), P("rows", "cols"),
        ),
        check_vma=False,
    )
```

```python
import functools

import jax
import jax.numpy as jnp
from jax import lax
from jax.experimental import pallas as pl
from jax.experimental.pallas import tpu as pltpu
from jax.sharding import PartitionSpec as P

MESH = pl.DeviceIdType.MESH

learn_rate = 0.01
decay_rate = 0.1
tiny_value = 1e-08

PARTS = 8
LATE = 3
SLAB = 64


def stepped(w, first, second):
    return w - learn_rate * (first / (jnp.sqrt(second) + tiny_value) + decay_rate * w)


def kernel(
    n_rows, n_cols, depth,
    w_g, f_g, s_g, w_u, f_u, s_u, norm_a, norm_b,
    ready, column, served, latest, late,
    held, sums, norms, in_sem, sum_send, sum_recv, norm_send, norm_recv, group_send, group_recv,
    send_sem, recv_sem,
):
    row, col = lax.axis_index("rows"), lax.axis_index("cols")
    z, y = row // 2, lax.rem(row, 2)
    across = z * 2 + (1 - y)
    half = z // 2
    is_outer = lax.rem(z + half, 2) == 0
    out_z, in_z = half * 3, 1 + half
    far_in_z, far_out_z = 2 - half, 3 - half * 3
    share, width = latest.shape[1], latest.shape[2] // PARTS
    pieces = 2 * PARTS
    me = row * n_cols + col
    sources = ((w_g, f_g, s_g), (w_u, f_u, s_u))

    def cols_of(k):
        if isinstance(k, int):
            return pl.ds((k % PARTS) * width, width)
        return pl.ds(pl.multiple_of(lax.rem(k, PARTS) * width, width), width)

    def load(k):
        copies = [
            pltpu.make_async_copy(
                ref.at[:, cols_of(k)], held.at[i, k // PARTS, :, cols_of(k)], in_sem.at[i, k]
            )
            for i, ref in enumerate(sources[k // PARTS])
        ]
        return copies

    for k in range(2):
        for c in load(k):
            c.start()

    barrier = pltpu.get_barrier_semaphore()

    def loop(lo, hi, f):
        def body(i, carry):
            f(i)
            return carry

        lax.fori_loop(lo, hi, body, 0)

    def row_peer(i):
        return lax.rem(row + i, n_rows)

    def col_peer(i):
        return lax.rem(col + i, n_cols)

    for i in range(1, n_rows):
        pl.semaphore_signal(barrier, inc=1, device_id=(row_peer(i), col), device_id_type=MESH)
    for i in range(1, n_cols):
        pl.semaphore_signal(barrier, inc=1, device_id=(row, col_peer(i)), device_id_type=MESH)

    lanes = norm_a.shape[1]
    norms[row, col] = jnp.zeros((1, 2 * lanes), jnp.float32)
    for side in range(2):

        @pl.when(lax.rem(me, 2) == side)
        def _():
            norms[row, col, :, side * lanes : (side + 1) * lanes] = norm_a[...] + norm_b[...]

    def adam(k):
        for c in load(k):
            c.wait()
        w, cs = k // PARTS, cols_of(k)

        def step(r, total):
            rs = pl.ds(pl.multiple_of(r * SLAB, SLAB), SLAB)
            new = stepped(held[0, w, rs, cs], held[1, w, rs, cs], held[2, w, rs, cs])
            latest[w, rs, cs] = new
            return total + jnp.sum(jnp.abs(new).reshape(SLAB // 8, 8, width), axis=0)

        total = lax.fori_loop(0, share // SLAB, step, jnp.zeros((8, width), jnp.float32))
        sums[k, row] = jnp.sum(total, axis=0, keepdims=True)

    def sum_copy(k, i):
        other = lax.rem(row + i, n_rows)
        return pltpu.make_async_remote_copy(
            src_ref=sums.at[k, row], dst_ref=sums.at[k, row],
            send_sem=sum_send.at[k, other], recv_sem=sum_recv.at[k, row],
            device_id=(other, col), device_id_type=MESH,
        )

    def sum_arrival(k, i):
        other = lax.rem(row + i, n_rows)
        return pltpu.make_async_remote_copy(
            src_ref=sums.at[k, other], dst_ref=sums.at[k, other],
            send_sem=sum_send.at[k, other], recv_sem=sum_recv.at[k, other],
            device_id=(other, col), device_id_type=MESH,
        )

    def scale(k):
        for i in range(1, n_rows):
            sum_arrival(k, i).wait_recv()
        w, cs = k // PARTS, cols_of(k)
        mean = jnp.sum(sums[k], axis=0) / depth
        column[w, :, cs] = mean

        def step(r, carry):
            rs = pl.ds(pl.multiple_of(r * SLAB, SLAB), SLAB)
            to = pl.ds(pl.multiple_of(row * share + r * SLAB, SLAB), SLAB)
            ready[w, to, cs] = (latest[w, rs, cs] / mean).astype(jnp.bfloat16)
            return carry

        lax.fori_loop(0, share // SLAB, step, 0)

    def block(source, k, link, slot, target):
        w = k // PARTS
        ref = ready.at[w, pl.ds(pl.multiple_of(source * share, share), share), cols_of(k)]
        return pltpu.make_async_remote_copy(
            src_ref=ref, dst_ref=ref,
            send_sem=send_sem.at[link, slot, k], recv_sem=recv_sem.at[source, k],
            device_id=(target, col), device_id_type=MESH,
        )

    def arrived(source, k):
        block(source, k, 0, 0, across).wait_recv()

    away = out_z * 2 + y
    near = in_z * 2 + y
    far_near, far_away = far_in_z * 2 + y, far_out_z * 2 + y
    near_across = in_z * 2 + (1 - y)
    away_across = out_z * 2 + (1 - y)
    far_near_across, far_away_across = far_in_z * 2 + (1 - y), far_out_z * 2 + (1 - y)

    partner = jnp.where(is_outer, near, away)

    def send_own(k):
        block(row, k, 1, 0, partner).start()
        block(row, k, 0, 0, across).start()

        @pl.when(jnp.logical_not(is_outer))
        def _():
            block(row, k, 2, 0, far_near).start()

    LAG = 4
    for k in range(pieces + LAG + 1):
        if k < pieces:
            if k + 2 < pieces:
                for c in load(k + 2):
                    c.start()
            adam(k)
        if k == 1:
            pl.semaphore_wait(barrier, n_rows + n_cols - 2)
        if 0 <= k - 1 - LAG:
            scale(k - 1 - LAG)
        if 1 <= k <= pieces:
            for i in range(1, n_rows):
                sum_copy(k - 1, i).start()
        if 0 <= k - 1 - LAG:
            send_own(k - 1 - LAG)

    def norm_copy(i, mine):
        at = col if mine else col_peer(i)
        return pltpu.make_async_remote_copy(
            src_ref=norms.at[row, at], dst_ref=norms.at[row, at],
            send_sem=norm_send.at[i], recv_sem=norm_recv.at[at],
            device_id=(row, col_peer(i)), device_id_type=MESH,
        )

    def group_copy(i, mine):
        at = row if mine else row_peer(i)
        return pltpu.make_async_remote_copy(
            src_ref=norms.at[at], dst_ref=norms.at[at],
            send_sem=group_send.at[i], recv_sem=group_recv.at[at],
            device_id=(row_peer(i), col), device_id_type=MESH,
        )

    for i in range(1, n_cols):
        norm_copy(i, True).start()
    for i in range(1, n_cols):
        norm_copy(i, False).wait_recv()
    for i in range(1, n_rows):
        group_copy(i, True).start()

    def keep(source):
        at = pl.ds(pl.multiple_of(source * share, share), share)
        late[...] = ready[1, at, (PARTS - LATE) * width : PARTS * width]

    @pl.when(is_outer)
    def _():
        def one(k):
            arrived(near, k)

            @pl.when(k < PARTS)
            def _():
                block(near, k, 0, 1, across).start()

            arrived(across, k)
            block(across, k, 1, 1, near).start()

        loop(0, pieces, one)

        def two(k):
            arrived(far_near, k)
            block(far_near, k, 0, 2, across).start()

        loop(0, pieces, two)

        def three(k):
            arrived(far_away, k)

            @pl.when(k < pieces - LATE)
            def _():
                block(far_away, k, 0, 3, across).start()

        loop(0, pieces, three)
        keep(far_away)

        def rest(k):
            arrived(far_near_across, k)

            @pl.when(k < pieces - LATE)
            def _():
                arrived(near_across, k)
                arrived(far_away_across, k)
                block(row, k, 0, 3, across).wait_send()

            for slot in (0, 2):
                block(row, k, 0, slot, across).wait_send()
            for slot in (0, 1):
                block(row, k, 1, slot, near).wait_send()

            @pl.when(k < PARTS)
            def _():
                block(row, k, 0, 1, across).wait_send()

        loop(0, pieces, rest)

    @pl.when(jnp.logical_not(is_outer))
    def _():
        def one(k):
            arrived(away, k)
            block(away, k, 2, 1, far_near).start()
            arrived(far_near, k)
            block(far_near, k, 1, 1, away).start()
            arrived(across, k)

        loop(0, pieces, one)

        def two(k):
            block(across, k, 2, 2, far_near).start()
            arrived(far_away, k)
            block(far_away, k, 1, 2, away).start()
            block(far_away, k, 0, 1, across).start()

        loop(0, pieces, two)
        loop(PARTS, pieces - LATE, lambda k: block(across, k, 1, 3, away).start())
        keep(across)

        def rest(k):
            arrived(away_across, k)
            arrived(far_near_across, k)
            arrived(far_away_across, k)
            for slot in (0, 1):
                block(row, k, 0, slot, across).wait_send()
            for slot in (0, 1, 2):
                block(row, k, 1, slot, away).wait_send()
                block(row, k, 2, slot, far_near).wait_send()

            @pl.when((k >= PARTS) & (k < pieces - LATE))
            def _():
                block(row, k, 1, 3, away).wait_send()

        loop(0, pieces, rest)

    for k in range(pieces):
        loop(1, n_rows, lambda i: sum_copy(k, i).wait_send())
    for i in range(1, n_cols):
        norm_copy(i, True).wait_send()
    for i in range(1, n_rows):
        group_copy(i, True).wait_send()
        group_copy(i, False).wait_recv()
    pairs = n_cols // 2
    for i in range(n_rows * pairs):
        r, c = i // pairs, 2 * (i % pairs)
        served[pl.ds(i, 1), :] = norms[r, c] + norms[r, c + 1]


def finish(ready, column, served, latest, *rest):
    outs, narrow, sem = rest[:7], rest[7], rest[8]
    narrow[...] = served[...].astype(jnp.bfloat16)
    copies = []
    cuts = 4
    rows = ready.shape[1] // cuts
    for w in range(2):
        for i in range(cuts):
            at = pl.ds(i * rows, rows)
            copies.append((ready.at[w, at], outs[w].at[at]))
        copies.append((latest.at[w], outs[5 + w]))
        copies.append((column.at[w], outs[2 + w]))
    copies.append((narrow, outs[4]))
    started = [pltpu.make_async_copy(a, b, sem.at[i]) for i, (a, b) in enumerate(copies)]
    for c in started:
        c.start()
    for c in started:
        c.wait()


def place(from_z, from_y, old, new, sem):
    row = lax.axis_index("rows")
    z, y = row // 2, lax.rem(row, 2)
    half = z // 2
    share, width = from_z.shape

    @pl.when(lax.rem(z + half, 2) == 0)
    def _():
        copies = []
        for i, (ref, at_z) in enumerate(((from_z, 1 + half), (from_y, 3 - half * 3))):
            start = pl.multiple_of((at_z * 2 + 1 - y) * share, share)
            to = new.at[pl.ds(start, share), pl.ds(new.shape[1] - width, width)]
            copies.append(pltpu.make_async_copy(ref, to, sem.at[i]))
        for c in copies:
            c.start()
        for c in copies:
            c.wait()


def fused(n_rows, n_cols, w_gate, first_gate, second_gate, w_up, first_up, second_up, norm_train, norm_step):
    share, width = w_gate.shape
    depth = share * n_rows
    pieces = 2 * PARTS
    lines = n_rows * n_cols // 2
    lanes = norm_train.shape[0]
    vmem = pl.BlockSpec(memory_space=pltpu.VMEM)
    hbm = pl.BlockSpec(memory_space=pltpu.HBM)
    dma = pltpu.SemaphoreType.DMA
    *found, late = pl.pallas_call(
        functools.partial(kernel, n_rows, n_cols, depth),
        out_shape=[
            pltpu.VMEM((2, depth, width), jnp.bfloat16),
            pltpu.VMEM((2, 1, width), jnp.float32),
            pltpu.VMEM((lines, 2 * lanes), jnp.float32),
            pltpu.VMEM((2, share, width), jnp.float32),
            pltpu.VMEM((share, LATE * (width // PARTS)), jnp.bfloat16),
        ],
        in_specs=[hbm] * 6 + [vmem] * 2,
        out_specs=[vmem] * 5,
        scratch_shapes=[
            pltpu.VMEM((3, 2, share, width), jnp.float32),
            pltpu.VMEM((pieces, n_rows, 1, width // PARTS), jnp.float32),
            pltpu.VMEM((n_rows, n_cols, 1, 2 * lanes), jnp.float32),
            dma((3, pieces)),
            dma((pieces, n_rows)),
            dma((pieces, n_rows)),
            dma((n_cols,)),
            dma((n_cols,)),
            dma((n_rows,)),
            dma((n_rows,)),
            dma((3, 4, pieces)),
            dma((n_rows, pieces)),
        ],
        compiler_params=pltpu.CompilerParams(
            collective_id=0, has_side_effects=True, vmem_limit_bytes=36 * 2**20
        ),
        name="fused",
    )(
        w_gate, first_gate, second_gate, w_up, first_up, second_up,
        norm_train.reshape(1, -1), norm_step.reshape(1, -1),
    )
    last = n_rows - 1
    from_z = lax.ppermute(late, "rows", [(2, 0), (3, 1), (last - 3, last - 1), (last - 2, last)])
    from_y = lax.ppermute(late, "rows", [(0, 1), (1, 0), (last - 1, last), (last, last - 1)])
    ready_gate, ready_up, column_gate, column_up, served, latest_gate, latest_up = pl.pallas_call(
        finish,
        out_shape=[jax.ShapeDtypeStruct((depth, width), jnp.bfloat16)] * 2
        + [jax.ShapeDtypeStruct((1, width), jnp.float32)] * 2
        + [jax.ShapeDtypeStruct((lines, 2 * lanes), jnp.bfloat16)]
        + [jax.ShapeDtypeStruct((share, width), jnp.float32)] * 2,
        in_specs=[vmem] * 4,
        out_specs=[hbm] * 7,
        scratch_shapes=[pltpu.VMEM((lines, 2 * lanes), jnp.bfloat16), dma((13,))],
        compiler_params=pltpu.CompilerParams(vmem_limit_bytes=2**20),
        cost_estimate=pl.CostEstimate(flops=0, bytes_accessed=40 * 2**20, transcendentals=0),
        name="finish",
    )(*found)
    ready_up = pl.pallas_call(
        place,
        out_shape=jax.ShapeDtypeStruct((depth, width), jnp.bfloat16),
        in_specs=[vmem] * 2 + [hbm],
        out_specs=hbm,
        input_output_aliases={2: 0},
        scratch_shapes=[dma((2,))],
        compiler_params=pltpu.CompilerParams(vmem_limit_bytes=2**20),
        name="place",
    )(from_z, from_y, ready_up)
    return (
        ready_gate, ready_up, column_gate.reshape(-1), column_up.reshape(-1), served.reshape(-1),
        latest_gate, latest_up,
    )


def plain(n_rows, n_cols, w_gate, first_gate, second_gate, w_up, first_up, second_up, norm_train, norm_step):
    latest = [stepped(w_gate, first_gate, second_gate), stepped(w_up, first_up, second_up)]
    totals = lax.psum(tuple(jnp.sum(jnp.abs(a), axis=0) for a in latest), "rows")
    columns = [t / (w_gate.shape[0] * n_rows) for t in totals]
    ready = [
        lax.all_gather((a / c).astype(jnp.bfloat16), "rows", axis=0, tiled=True)
        for a, c in zip(latest, columns)
    ]
    served = lax.all_gather(
        (norm_train + norm_step).astype(jnp.bfloat16), ("rows", "cols"), axis=0, tiled=True
    )
    return (*ready, *columns, served, *latest)


def solution(mesh):
    n_rows, n_cols = mesh.shape["rows"], mesh.shape["cols"]
    body = fused if (n_rows, n_cols) == (8, 4) else plain
    placed = (P("rows", "cols"),) * 6 + (P(("rows", "cols")),) * 2
    return jax.shard_map(
        functools.partial(body, n_rows, n_cols),
        mesh=mesh,
        in_specs=placed,
        out_specs=(
            P(None, "cols"), P(None, "cols"), P("cols"), P("cols"), P(),
            P("rows", "cols"), P("rows", "cols"),
        ),
        check_vma=False,
    )
```
